32 devices in a mesh: members: 2 (over x), zonal: 8 (over z, y), merid: 2 (over core).
Axes of the slice: x: 2, y: 2, z: 4, core: 2. Of those that a mesh axis runs over, the one named last changes fastest.
Arguments:
- height: float32 [256, 1024], P(('members', 'zonal'), 'merid'), parts along dimension 0, may hold values from -6 to 6
- transport_u: float32 [256, 1024], P(('members', 'zonal'), 'merid'), parts along dimension 0, may hold values from -4 to 4
- transport_v: float32 [256, 1024], P(('members', 'zonal'), 'merid'), parts along dimension 0, may hold values from -4 to 4
- thickness: float32 [14, 256, 1024], P(None, ('members', 'zonal'), 'merid'), parts along dimension 1, may hold values from 0.5 to 2
- velocity_u: float32 [14, 256, 1024], P(None, ('members', 'zonal'), 'merid'), parts along dimension 1, may hold values from -3 to 3
- velocity_v: float32 [14, 256, 1024], P(None, ('members', 'zonal'), 'merid'), parts along dimension 1, may hold values from -3 to 3
- sea_faces: int32 [2, 128, 1024], P(None, 'zonal', 'merid'), may hold values 0 or 1
- wind_seeds: int32 [8, 2], P('members'), parts along dimension 0, may hold values from 1 to 96
- wind_scale: float32 [8], P('members'), parts along dimension 0, may hold values from 0.5 to 2
- wind_base: float32 [2, 128, 1024], P(None, 'zonal', 'merid'), may hold values from -6 to 6
Outputs:
- final_height: float32 [256, 1024], P(('members', 'zonal'), 'merid'), parts along dimension 0
- final_transport_u: float32 [256, 1024], P(('members', 'zonal'), 'merid'), parts along dimension 0
- final_transport_v: float32 [256, 1024], P(('members', 'zonal'), 'merid'), parts along dimension 0
- final_thickness: float32 [14, 256, 1024], P(None, ('members', 'zonal'), 'merid'), parts along dimension 1
- final_velocity_u: float32 [14, 256, 1024], P(None, ('members', 'zonal'), 'merid'), parts along dimension 1
- final_velocity_v: float32 [14, 256, 1024], P(None, ('members', 'zonal'), 'merid'), parts along dimension 1
The draws below stay inside these ranges and needn't reach their ends.
There are 2 independent parts, one for each index of `members`. The reference program is written for one: setup_inputs(seed, part) draws one part's arguments, and reference() takes and returns one part's arrays. A program takes and returns all parts, laid end to end along the dimension named above; an argument that names none is the same for every part. Nothing has to cross between parts.
All inputs are finite; a program needn't handle non-finite values. No bound on the sum of `sea_faces` on one device may be relied on, other than what follows from the above.
Results may differ from the reference program's by a relative error of at most 0.0001.
Values sent between devices are 32-bit elements; how exact they have to be, the bound alone decides.
A program may use at most 64 MiB of HBM per device.

```python
import math
import jax
import jax.numpy as jnp

LAYERS = 14
NSUB = 6
STEPS = 2
MODES = 4
NX = 128
NY = 1024


def plant(result, stream_key, least, top_value):
    spot = [jax.random.randint(jax.random.fold_in(stream_key, axis), (), 0, length) for axis, length in enumerate(result.shape)]
    widest = result.shape.index(max(result.shape))
    beside = spot[:widest] + [(spot[widest] + 1) % result.shape[widest]] + spot[widest + 1:]
    return result.at[tuple(spot)].set(least).at[tuple(beside)].set(top_value)


def block_scale(own_key, extent, shards, least, largest):
    def one(dim, blocks):
        heights = jax.random.uniform(jax.random.fold_in(jax.random.fold_in(own_key, 6), dim), (blocks,), jnp.float32, least / len(shards), largest / len(shards))
        return jnp.repeat(jnp.exp(heights), extent[dim] // blocks).reshape((-1,) + (1,) * (len(extent) - dim - 1))

    gain = one(*shards[0])
    for cut in shards[1:]:
        gain = gain * one(*cut)
    return gain


def noise(rng, shape, deviation, limit, split=(), kind=jnp.bfloat16):
    gain = block_scale(rng, shape, split, -0.22, 0.18) if split else 1.0
    entries = jax.random.normal(rng, shape, jnp.float32) * deviation * gain
    return jnp.minimum(jnp.maximum(entries, -limit), limit).astype(kind)


def setup_inputs(seed: int = 0, part: int = 0) -> dict:
    splits = jax.random.split(jax.random.key(seed), 11)
    part_splits = jax.random.split(jax.random.fold_in(splits[10], part), 11)
    return {
        "height": noise(part_splits[0], (NX, NY), 1.0, 6.0, ((0, 8), (1, 2)), jnp.float32),
        "transport_u": noise(part_splits[1], (NX, NY), 0.5, 4.0, ((0, 8), (1, 2)), jnp.float32),
        "transport_v": noise(part_splits[2], (NX, NY), 0.5, 4.0, ((0, 8), (1, 2)), jnp.float32),
        "thickness": jnp.clip(jnp.exp(math.log(2.0) - 1.3862944 * jax.random.uniform(part_splits[3], (LAYERS, NX, NY), jnp.float32) ** block_scale(part_splits[3], (LAYERS, NX, NY), ((1, 8), (2, 2)), -0.2, 0.2)), 0.5, 2.0),
        "velocity_u": noise(part_splits[4], (LAYERS, NX, NY), 0.5, 3.0, ((1, 8), (2, 2)), jnp.float32),
        "velocity_v": noise(part_splits[5], (LAYERS, NX, NY), 0.5, 3.0, ((1, 8), (2, 2)), jnp.float32),
        "sea_faces": plant((jax.random.randint(splits[6], (2, NX, NY), 0, 8) < 7).astype(jnp.int32), jax.random.fold_in(splits[6], 1), 0, 1),
        "wind_seeds": plant(jax.random.randint(part_splits[7], (MODES, 2), 1, 97), jax.random.fold_in(part_splits[7], 1), 1, 96).astype(jnp.int32),
        "wind_scale": jnp.clip(jnp.exp(jax.random.uniform(part_splits[8], (MODES,), jnp.float32, math.log(0.5), math.log(2.0))), 0.5, 2.0),
        "wind_base": noise(splits[9], (2, NX, NY), 1.0, 6.0, ((1, 8), (2, 2)), jnp.float32),
    }


WAVE_LIMIT = 0.225
STRESS_SCALE = 0.1
FLUX_STEP = 0.05
PRESS_COEF = 0.05


def east(field):
    return jnp.roll(field, -1, axis=-2)


def west(field):
    return jnp.roll(field, 1, axis=-2)


def north(field):
    folded = jnp.flip(field[..., -1], axis=-1)
    return jnp.concatenate([field[..., 1:], folded[..., None]], axis=-1)


def south(field):
    return jnp.concatenate([jnp.zeros_like(field[..., :1]), field[..., :-1]], axis=-1)


def reference(height, transport_u, transport_v, thickness, velocity_u, velocity_v, sea_faces, wind_seeds, wind_scale, wind_base):
    total_x = height.shape[0]
    total_y = height.shape[1]
    mask_u = sea_faces[0].astype(jnp.float32)
    mask_v = sea_faces[1].astype(jnp.float32)
    columns = jnp.arange(total_x, dtype=jnp.int32)
    rows_idx = jnp.arange(total_y, dtype=jnp.int32)
    wave_x = wind_seeds[:, 0].astype(jnp.int32)
    wave_y = wind_seeds[:, 1].astype(jnp.int32)
    phase = ((wave_x[:, None, None] * columns[None, :, None]) % total_x).astype(jnp.float32) / total_x
    phase = phase + ((wave_y[:, None, None] * rows_idx[None, None, :]) % total_y).astype(jnp.float32) / total_y
    angle = (2.0 * math.pi) * phase
    amplitude = wind_scale[:, None, None]
    stress_x = STRESS_SCALE * (wind_base[0] + jnp.sum(amplitude * jnp.cos(angle), axis=0))
    stress_y = STRESS_SCALE * (wind_base[1] + jnp.sum(amplitude * jnp.sin(angle), axis=0))
    layers = thickness.shape[0]
    wave = (WAVE_LIMIT / layers) * jnp.sum(thickness, axis=0)
    depth_u = jnp.sum((thickness + east(thickness)) * 0.5, axis=0)
    depth_v = jnp.sum((thickness + north(thickness)) * 0.5, axis=0)
    surface, flow_u, flow_v = height, transport_u, transport_v
    thick, speed_u, speed_v = thickness, velocity_u, velocity_v
    for outer in range(STEPS):
        mean_u = jnp.zeros_like(surface)
        mean_v = jnp.zeros_like(surface)
        for inner in range(NSUB):
            surface = surface - (flow_u - west(flow_u) + flow_v - south(flow_v))
            flow_u = mask_u * (flow_u - wave * (east(surface) - surface) + stress_x)
            flow_v = mask_v * (flow_v - wave * (north(surface) - surface) + stress_y)
            mean_u = mean_u + flow_u
            mean_v = mean_v + flow_v
        mean_u = mean_u / NSUB
        mean_v = mean_v / NSUB
        thick_u = (thick + east(thick)) * 0.5
        thick_v = (thick + north(thick)) * 0.5
        flux_u = speed_u * thick_u
        flux_v = speed_v * thick_v
        pressure = jnp.cumsum(thick, axis=0)
        trial_u = speed_u - PRESS_COEF * (east(pressure) - pressure)
        trial_v = speed_v - PRESS_COEF * (north(pressure) - pressure)
        speed_u = mask_u * (trial_u + (mean_u - jnp.sum(thick_u * trial_u, axis=0)) / depth_u)
        speed_v = mask_v * (trial_v + (mean_v - jnp.sum(thick_v * trial_v, axis=0)) / depth_v)
        thick = thick - FLUX_STEP * (flux_u - west(flux_u) + flux_v - south(flux_v))
    return surface, flow_u, flow_v, thick, speed_u, speed_v
```

```python
import functools
import math

import jax
import jax.numpy as jnp
from jax import lax
from jax.experimental import pallas as pl
from jax.experimental.pallas import tpu as pltpu
from jax.sharding import PartitionSpec as P

NSUB = 6
STEPS = 2
MARGIN = NSUB * STEPS

WAVE_LIMIT = 0.225
STRESS_SCALE = 0.1
FLUX_STEP = 0.05
PRESS_COEF = 0.05
LANES = 128
FIELDS = 8
SLOT = LANES // FIELDS
MESH = pl.DeviceIdType.MESH


def roll(value, shift, axis):
    return pltpu.roll(value, shift % value.shape[axis], axis)


def iota(shape, axis):
    return lax.broadcasted_iota(jnp.int32, shape, axis)


def turns(seed, index, total):
    part = seed * index * (1.0 / total)
    angle = (2.0 * math.pi) * (part - jnp.floor(part))
    return jnp.cos(angle), jnp.sin(angle)


def kernel(
    zonal_devices,
    merid_devices,
    height,
    trans_u,
    trans_v,
    thick,
    vel_u,
    vel_v,
    faces,
    seeds,
    scale,
    base,
    o_eta,
    o_bu,
    o_bv,
    o_h,
    o_u,
    o_v,
    X,
    G,
    wind_own,
    wind_far,
    half_send,
    half_recv,
    pack_send,
    inner_recv,
    fold_recv,
    mean,
    depth,
    lay_send_r,
    lay_send_l,
    lay_recv_w,
    lay_recv_e,
    lay_pack_send,
    lay_pack_recv,
    send_sem,
    recv_sem,
    lay_send_sem,
    lay_recv_sem,
):
    layers, nx, ny = thick.shape
    Z = zonal_devices
    total_x, total_y = nx * Z, ny * merid_devices
    z = lax.axis_index("zonal")
    m = lax.axis_index("merid")
    other = 1 - m
    bottom = m == 0
    top = m == merid_devices - 1
    right, left = lax.rem(z + 1, Z), lax.rem(z + Z - 1, Z)
    mirror = Z - 1 - z
    mirror_e, mirror_w = lax.rem(mirror + 1, Z), lax.rem(mirror + Z - 1, Z)
    extra = MARGIN - 8
    rows = 3 * nx
    width = ny + LANES
    last = ny - LANES

    barrier = pltpu.get_barrier_semaphore()
    for zz, mm in ((left, m), (right, m), (left, other), (right, other), (z, other)):
        pl.semaphore_signal(barrier, inc=1, device_id={"zonal": zz, "merid": mm}, device_id_type=MESH)
    for zz in (mirror_w, mirror, mirror_e):

        @pl.when(jnp.logical_and(top, zz != z))
        def _():
            pl.semaphore_signal(barrier, inc=1, device_id={"zonal": zz}, device_id_type=MESH)

    own = slice(nx, 2 * nx)
    X[0, own, 0:ny] = height[...]
    X[1, own, 0:ny] = trans_u[...]
    X[2, own, 0:ny] = trans_v[...]
    X[3, own, 0:ny] = faces[0].astype(jnp.float32)
    X[4, own, 0:ny] = faces[1].astype(jnp.float32)
    total = thick[0]
    for l in range(1, layers):
        total = total + thick[l]
    X[5, own, 0:ny] = (WAVE_LIMIT / layers) * total
    X[6, own, 0:ny] = base[0]
    X[7, own, 0:ny] = base[1]
    for f in range(FIELDS):
        half_send[0, f * extra : (f + 1) * extra, :] = X[f, 2 * nx - MARGIN : 2 * nx - 8, 0:ny]
        half_send[1, f * extra : (f + 1) * extra, :] = X[f, nx + 8 : nx + MARGIN, 0:ny]
    lane = iota((nx, LANES), 1)
    inner = jnp.zeros((nx, LANES), jnp.float32)
    crest = jnp.zeros((nx, LANES), jnp.float32)
    for f in range(FIELDS):
        here = jnp.logical_and(lane >= f * SLOT, lane < (f + 1) * SLOT)
        high = roll(X[f, own, last:ny], SLOT * (f + 1), 1)
        low = roll(X[f, own, 0:LANES], SLOT * f, 1)
        crest = jnp.where(here, high, crest)
        inner = jnp.where(here, jnp.where(bottom, high, low), inner)
    pack_send[0] = inner
    pack_send[2] = crest
    for r in range(nx):
        pack_send[1, r : r + 1, :] = pack_send[2, nx - 1 - r : nx - r, :]

    across = sum((zz != z).astype(jnp.int32) for zz in (mirror_w, mirror, mirror_e))
    pl.semaphore_wait(barrier, 5 + jnp.where(top, across, 0))

    def send(src, dst, k, zz, mm):
        return pltpu.make_async_remote_copy(
            src_ref=src,
            dst_ref=dst,
            send_sem=send_sem.at[k],
            recv_sem=recv_sem.at[k],
            device_id={"zonal": zz, "merid": mm},
            device_id_type=MESH,
        )

    copies = [
        send(X.at[:, nx : nx + 8, 0:ny], X.at[:, 2 * nx : 2 * nx + 8, 0:ny], 0, left, m),
        send(X.at[:, 2 * nx - 8 : 2 * nx, 0:ny], X.at[:, nx - 8 : nx, 0:ny], 1, right, m),
        send(half_send.at[0], half_recv.at[0], 2, right, m),
        send(half_send.at[1], half_recv.at[1], 3, left, m),
        send(pack_send.at[0], inner_recv.at[2], 4, left, other),
        send(pack_send.at[0], inner_recv.at[1], 5, z, other),
        send(pack_send.at[0], inner_recv.at[0], 6, right, other),
    ]
    folds = [
        (send(pack_send.at[1], fold_recv.at[s], 7 + s, zz, m),
         pltpu.make_async_copy(pack_send.at[1], fold_recv.at[s], recv_sem.at[7 + s]), zz)
        for s, zz in ((2, mirror_w), (1, mirror), (0, mirror_e))
    ]
    for copy in copies[4:]:
        copy.start()
    for far_copy, near_copy, zz in folds:

        @pl.when(jnp.logical_and(top, zz != z))
        def _():
            far_copy.start()

        @pl.when(jnp.logical_and(top, zz == z))
        def _():
            near_copy.start()

    for copy in copies[:4]:
        copy.start()

    def lay_copies(step):
        def one(src, dst, k, zz, mm):
            return pltpu.make_async_remote_copy(
                src_ref=src,
                dst_ref=dst,
                send_sem=lay_send_sem.at[step, k],
                recv_sem=lay_recv_sem.at[step, k],
                device_id={"zonal": zz, "merid": mm},
                device_id_type=MESH,
            )

        return [
            one(lay_send_r.at[step], lay_recv_w.at[step], 0, right, m),
            one(lay_send_l.at[step], lay_recv_e.at[step], 1, left, m),
            one(lay_pack_send.at[step, 0], lay_pack_recv.at[step, 0], 2, z, other),
            one(lay_pack_send.at[step, 1], lay_pack_recv.at[step, 1], 3, mirror, m),
        ]

    above = lay_send_r.shape[1] // 2

    def send_layers(step, h_ref, u_ref, v_ref):
        edge = jnp.zeros((nx, LANES), jnp.float32)
        brim = jnp.zeros((nx, LANES), jnp.float32)
        for l in range(layers):
            lay_send_r[step, l : l + 1, :] = h_ref[l, nx - 1 : nx, :]
            lay_send_r[step, above + l : above + l + 1, :] = u_ref[l, nx - 1 : nx, :]
            lay_send_l[step, l : l + 1, :] = h_ref[l, 0:1, :]
            high = roll(h_ref[l, :, last:ny], l + 1, 1)
            low = roll(h_ref[l, :, 0:LANES], l, 1)
            high_v = roll(v_ref[l, :, last:ny], layers + l + 1, 1)
            edge = jnp.where(lane == l, jnp.where(bottom, high, low), edge)
            edge = jnp.where(lane == layers + l, high_v, edge)
            brim = jnp.where(lane == l, high, brim)
        lay_pack_send[step, 0] = edge
        lay_pack_send[step, 2] = brim
        for r in range(nx):
            lay_pack_send[step, 1, r : r + 1, :] = lay_pack_send[step, 2, nx - 1 - r : nx - r, :]
        out = lay_copies(step)
        for copy in out[:3]:
            copy.start()

        @pl.when(top)
        def _():
            out[3].start()

        return out

    def wait_layers(out):
        for copy in out[:3]:
            copy.wait()

        @pl.when(top)
        def _():
            out[3].wait()

    out = send_layers(0, thick, vel_u, vel_v)

    first = (z * nx - nx).astype(jnp.float32)
    col = first + iota((rows, 1), 0).astype(jnp.float32) + float(total_x)
    far_col = float(2 * total_x - 1) - (first + iota((rows, 1), 0).astype(jnp.float32))
    spot = iota((1, width), 1)
    row = spot + m * ny
    row = jnp.where(jnp.logical_and(top, spot >= ny), row - width, row).astype(jnp.float32)
    far_row = (iota((1, LANES), 1) + (total_y - LANES)).astype(jnp.float32)
    px = jnp.zeros((rows, width), jnp.float32)
    py = jnp.zeros((rows, width), jnp.float32)
    fx = jnp.zeros((rows, LANES), jnp.float32)
    fy = jnp.zeros((rows, LANES), jnp.float32)
    for k in range(seeds.shape[0]):
        seed_x = seeds[k, 0].astype(jnp.float32)
        seed_y = seeds[k, 1].astype(jnp.float32)
        ca, sa = turns(seed_x, col, total_x)
        cf, sf = turns(seed_x, far_col, total_x)
        cb, sb = turns(seed_y, row, total_y)
        cg, sg = turns(seed_y, far_row, total_y)
        amp = scale[k]
        ca, sa, cf, sf = amp * ca, amp * sa, amp * cf, amp * sf
        px = px + (ca * cb - sa * sb)
        py = py + (sa * cb + ca * sb)
        fx = fx + (cf * cg - sf * sg)
        fy = fy + (sf * cg + cf * sg)
    wind_own[0] = px
    wind_own[1] = py
    wind_far[0] = fx
    wind_far[1] = fy

    for copy in copies:
        copy.wait()
    for far_copy, near_copy, zz in folds:

        @pl.when(jnp.logical_and(top, zz != z))
        def _():
            far_copy.wait()

        @pl.when(jnp.logical_and(top, zz == z))
        def _():
            near_copy.wait()

    for f in range(FIELDS):
        X[f, nx - MARGIN : nx - 8, 0:ny] = half_recv[0, f * extra : (f + 1) * extra, :]
        X[f, 2 * nx + 8 : 2 * nx + MARGIN, 0:ny] = half_recv[1, f * extra : (f + 1) * extra, :]
        for s in range(3):
            got = inner_recv[s]
            part = slice(s * nx, (s + 1) * nx)
            X[f, part, ny:width] = jnp.where(
                top, roll(got, LANES - SLOT * (f + 1), 1), roll(got, LANES - SLOT * f, 1)
            )
            G[f, part, :] = roll(fold_recv[s], LANES - SLOT * (f + 1), 1)
    for k in range(2):
        X[6 + k] = STRESS_SCALE * (X[6 + k] + wind_own[k])
        G[6 + k] = STRESS_SCALE * (G[6 + k] + wind_far[k])

    lanes = iota((rows, width), 1)
    wall = jnp.logical_and(bottom, lanes == 0)
    crown = jnp.logical_and(top, lanes == ny - 1)
    far_top = iota((rows, LANES), 1) == LANES - 1

    def substep(_, carry):
        eta, bu, bv = X[0], X[1], X[2]
        g_eta, g_bu, g_bv = G[0], G[1], G[2]
        eta = eta - (bu - roll(bu, 1, 0) + bv - jnp.where(wall, 0.0, roll(bv, 1, 1)))
        g_eta = g_eta - (g_bu - roll(g_bu, -1, 0) + g_bv - roll(g_bv, 1, 1))
        north = jnp.where(crown, g_eta[:, LANES - 1 :], roll(eta, -1, 1))
        g_north = jnp.where(far_top, eta[:, ny - 1 : ny], roll(g_eta, -1, 1))
        bu = X[3] * (bu - X[5] * (roll(eta, -1, 0) - eta) + X[6])
        bv = X[4] * (bv - X[5] * (north - eta) + X[7])
        g_bu = G[3] * (g_bu - G[5] * (roll(g_eta, 1, 0) - g_eta) + G[6])
        g_bv = G[4] * (g_bv - G[5] * (g_north - g_eta) + G[7])
        X[0], X[1], X[2] = eta, bu, bv
        G[0], G[1], G[2] = g_eta, g_bu, g_bv
        mean[0] = mean[0] + bu[nx : 2 * nx, 0:ny]
        mean[1] = mean[1] + bv[nx : 2 * nx, 0:ny]
        return carry

    def substeps():
        mean[...] = jnp.zeros_like(mean)
        lax.fori_loop(0, NSUB, substep, 0)

    row_id = iota((nx, ny), 0)
    lane_id = iota((nx, ny), 1)
    at_west = row_id == 0
    at_east = row_id == nx - 1
    at_south = lane_id == 0
    at_north = lane_id == ny - 1

    def layer_step(step, h_ref, u_ref, v_ref):
        zero = jnp.zeros((nx, ny), jnp.float32)
        press_u, press_v, sum_u, sum_v = zero, zero, zero, zero
        deep_u, deep_v = zero, zero
        for l in range(layers):
            h, u, v = h_ref[l], u_ref[l], v_ref[l]
            side = lay_pack_recv[step, 0, :, l : l + 1]
            cap = jnp.where(top, lay_pack_recv[step, 1, :, l : l + 1], side)
            south_v = lay_pack_recv[step, 0, :, layers + l : layers + l + 1]
            h_east = jnp.where(at_east, lay_recv_e[step, l : l + 1, :], roll(h, -1, 0))
            h_north = jnp.where(at_north, cap, roll(h, -1, 1))
            hu = (h + h_east) * 0.5
            hv = (h + h_north) * 0.5
            if step == 0:
                deep_u = deep_u + hu
                deep_v = deep_v + hv
            flux_u = u * hu
            flux_v = v * hv
            west_row = lay_recv_w[step, above + l : above + l + 1, :] * (
                (lay_recv_w[step, l : l + 1, :] + h[0:1, :]) * 0.5
            )
            south_col = jnp.where(top, south_v * ((side + h[:, 0:1]) * 0.5), 0.0)
            flux_w = jnp.where(at_west, west_row, roll(flux_u, 1, 0))
            flux_s = jnp.where(at_south, south_col, roll(flux_v, 1, 1))
            press_u = press_u + (h_east - h)
            press_v = press_v + (h_north - h)
            trial_u = u - PRESS_COEF * press_u
            trial_v = v - PRESS_COEF * press_v
            sum_u = sum_u + hu * trial_u
            sum_v = sum_v + hv * trial_v
            o_u[l] = trial_u
            o_v[l] = trial_v
            o_h[l] = h - FLUX_STEP * (flux_u - flux_w + flux_v - flux_s)
        if step == 0:
            depth[0] = 1.0 / deep_u
            depth[1] = 1.0 / deep_v
        fix_u = (mean[0] * (1.0 / NSUB) - sum_u) * depth[0]
        fix_v = (mean[1] * (1.0 / NSUB) - sum_v) * depth[1]
        mask_u, mask_v = X[3, own, 0:ny], X[4, own, 0:ny]
        for l in range(layers):
            o_u[l] = mask_u * (o_u[l] + fix_u)
            o_v[l] = mask_v * (o_v[l] + fix_v)

    substeps()
    wait_layers(out)
    layer_step(0, thick, vel_u, vel_v)
    for step in range(1, STEPS):
        out = send_layers(step, o_h, o_u, o_v)
        substeps()
        wait_layers(out)
        layer_step(step, o_h, o_u, o_v)
    o_eta[...] = X[0, own, 0:ny]
    o_bu[...] = X[1, own, 0:ny]
    o_bv[...] = X[2, own, 0:ny]


def body(zonal_devices, merid_devices, *args):
    height, _, _, thickness = args[:4]
    layers, nx, ny = thickness.shape
    up = -(-layers // 8) * 8
    f32 = jnp.float32
    vmem = pl.BlockSpec(memory_space=pltpu.VMEM)
    smem = pl.BlockSpec(memory_space=pltpu.SMEM)
    extra = FIELDS * (MARGIN - 8)
    plane = jax.ShapeDtypeStruct((nx, ny), f32)
    solid = jax.ShapeDtypeStruct((layers, nx, ny), f32)
    return pl.pallas_call(
        functools.partial(kernel, zonal_devices, merid_devices),
        out_shape=(plane, plane, plane, solid, solid, solid),
        in_specs=[vmem] * 7 + [smem] * 2 + [vmem],
        out_specs=[vmem] * 6,
        scratch_shapes=[
            pltpu.VMEM((FIELDS, 3 * nx, ny + LANES), f32),
            pltpu.VMEM((FIELDS, 3 * nx, LANES), f32),
            pltpu.VMEM((2, 3 * nx, ny + LANES), f32),
            pltpu.VMEM((2, 3 * nx, LANES), f32),
            pltpu.VMEM((2, extra, ny), f32),
            pltpu.VMEM((2, extra, ny), f32),
            pltpu.VMEM((3, nx, LANES), f32),
            pltpu.VMEM((3, nx, LANES), f32),
            pltpu.VMEM((3, nx, LANES), f32),
            pltpu.VMEM((2, nx, ny), f32),
            pltpu.VMEM((2, nx, ny), f32),
            pltpu.VMEM((STEPS, 2 * up, ny), f32),
            pltpu.VMEM((STEPS, up, ny), f32),
            pltpu.VMEM((STEPS, 2 * up, ny), f32),
            pltpu.VMEM((STEPS, up, ny), f32),
            pltpu.VMEM((STEPS, 3, nx, LANES), f32),
            pltpu.VMEM((STEPS, 2, nx, LANES), f32),
            pltpu.SemaphoreType.DMA((10,)),
            pltpu.SemaphoreType.DMA((10,)),
            pltpu.SemaphoreType.DMA((STEPS, 4)),
            pltpu.SemaphoreType.DMA((STEPS, 4)),
        ],
        compiler_params=pltpu.CompilerParams(
            collective_id=0, has_side_effects=True, vmem_limit_bytes=60 * 1024 * 1024
        ),
        name="ocean",
    )(*args)


def solution(mesh):
    field = P(("members", "zonal"), "merid")
    solid = P(None, ("members", "zonal"), "merid")
    fixed = P(None, "zonal", "merid")
    return jax.shard_map(
        functools.partial(body, mesh.shape["zonal"], mesh.shape["merid"]),
        mesh=mesh,
        in_specs=(
            field, field, field, solid, solid, solid, fixed, P("members", None), P("members"), fixed,
        ),
        out_specs=(field, field, field, solid, solid, solid),
        check_vma=False,
    )
```

```python
import functools
import math

import jax
import jax.numpy as jnp
from jax import lax
from jax.experimental import pallas as pl
from jax.experimental.pallas import tpu as pltpu
from jax.sharding import PartitionSpec as P

NSUB = 6
STEPS = 2
MARGIN = NSUB
PAD = 8

WAVE_LIMIT = 0.225
STRESS_SCALE = 0.1
FLUX_STEP = 0.05
PRESS_COEF = 0.05
LANES = 128
VMEM_BYTES = 67043328
SPARE = 1 << 15
FIELDS = 8
SLOT = LANES // FIELDS
WEST = (NSUB - 1, NSUB, NSUB - 1, NSUB - 1, NSUB - 2, NSUB - 1, NSUB - 1, NSUB - 2)
EAST = (NSUB, NSUB, NSUB) + (NSUB - 1,) * 5
MESH = pl.DeviceIdType.MESH


def roll(value, shift, axis):
    return pltpu.roll(value, shift % value.shape[axis], axis)


def iota(shape, axis):
    return lax.broadcasted_iota(jnp.int32, shape, axis)


def turns(seed, index, total):
    part = seed * index * (1.0 / total)
    angle = (2.0 * math.pi) * (part - jnp.floor(part))
    return jnp.cos(angle), jnp.sin(angle)


def tile_up(count):
    return -(-count // 8) * 8


def layer_step(h_ref, u_ref, v_ref, recv_w, recv_e, packs, mean, mask_u, mask_v, depth, o_h, o_u, o_v, top, deep, sent):
    layers, nx, ny = h_ref.shape
    above = recv_w.shape[0] // 2
    row_id = iota((nx, ny), 0)
    lane_id = iota((nx, ny), 1)
    at_west = row_id == 0
    at_east = row_id == nx - 1
    at_south = lane_id == 0
    at_north = lane_id == ny - 1
    zero = jnp.zeros((nx, ny), jnp.float32)
    press_u, press_v, sum_u, sum_v = zero, zero, zero, zero
    deep_u, deep_v = zero, zero
    for l in range(layers):
        h, u, v = h_ref[l], u_ref[l], v_ref[l]
        side = packs[0, :, l : l + 1]
        cap = jnp.where(top, packs[1, :, l : l + 1], side)
        south_v = packs[0, :, layers + l : layers + l + 1]
        h_east = jnp.where(at_east, recv_e[l : l + 1, :], roll(h, -1, 0))
        h_north = jnp.where(at_north, cap, roll(h, -1, 1))
        hu = (h + h_east) * 0.5
        hv = (h + h_north) * 0.5
        if deep:
            deep_u = deep_u + hu
            deep_v = deep_v + hv
        flux_u = u * hu
        flux_v = v * hv
        west_row = recv_w[above + l : above + l + 1, :] * ((recv_w[l : l + 1, :] + h[0:1, :]) * 0.5)
        south_col = jnp.where(top, south_v * ((side + h[:, 0:1]) * 0.5), 0.0)
        flux_w = jnp.where(at_west, west_row, roll(flux_u, 1, 0))
        flux_s = jnp.where(at_south, south_col, roll(flux_v, 1, 1))
        press_u = press_u + (h_east - h)
        press_v = press_v + (h_north - h)
        trial_u = u - PRESS_COEF * press_u
        trial_v = v - PRESS_COEF * press_v
        sum_u = sum_u + hu * trial_u
        sum_v = sum_v + hv * trial_v
        o_u[l] = trial_u
        o_v[l] = trial_v
        o_h[l] = h - FLUX_STEP * (flux_u - flux_w + flux_v - flux_s)
    sent(0)
    if deep:
        depth[0] = 1.0 / deep_u
        depth[1] = 1.0 / deep_v
    fix_u = (mean[0] * (1.0 / NSUB) - sum_u) * depth[0]
    fix_v = (mean[1] * (1.0 / NSUB) - sum_v) * depth[1]
    for l in range(layers):
        o_u[l] = mask_u * (o_u[l] + fix_u)
    sent(1)
    for l in range(layers):
        o_v[l] = mask_v * (o_v[l] + fix_v)
    sent(2)


def last_kernel(
    aux, h_ref, u_ref, v_ref, recv_w, recv_e, packs, o_eta, o_bu, o_bv, o_h, o_u, o_v, n_h, n_u, n_v, sems
):
    top = lax.axis_index("merid") == lax.axis_size("merid") - 1
    flat = [pltpu.make_async_copy(aux.at[k], o, sems.at[3 + k]) for k, o in enumerate((o_eta, o_bu, o_bv))]
    for copy in flat:
        copy.start()
    out = [pltpu.make_async_copy(n, o, sems.at[k]) for k, (n, o) in enumerate(((n_h, o_h), (n_u, o_u), (n_v, o_v)))]
    layer_step(
        h_ref, u_ref, v_ref, recv_w, recv_e, packs, aux.at[3:5], aux[7], aux[8], aux.at[5:7],
        n_h, n_u, n_v, top, False, lambda k: out[k].start(),
    )
    for copy in flat + out:
        copy.wait()


def kernel(
    zonal_devices,
    merid_devices,
    height_any,
    trans_u_any,
    trans_v_any,
    thick_any,
    vel_u_any,
    vel_v_any,
    faces_any,
    seeds_any,
    scale_any,
    base_any,
    aux,
    o_h,
    o_u,
    o_v,
    o_recv_w,
    o_recv_e,
    o_packs,
    thick,
    vel_u,
    vel_v,
    faces,
    seeds,
    scale,
    X,
    G,
    wind_own,
    wind_far,
    west_send,
    west_recv,
    east_send,
    east_recv,
    pack_send,
    inner_recv,
    fold_recv,
    lay_send_r,
    lay_send_l,
    lay_recv_w,
    lay_recv_e,
    lay_pack_send,
    lay_pack_recv,
    load_sem,
    send_sem,
    recv_sem,
    lay_send_sem,
    lay_recv_sem,
):
    layers, nx, ny = thick.shape
    Z = zonal_devices
    total_x, total_y = nx * Z, ny * merid_devices
    z = lax.axis_index("zonal")
    m = lax.axis_index("merid")
    other = 1 - m
    bottom = m == 0
    top = m == merid_devices - 1
    right, left = lax.rem(z + 1, Z), lax.rem(z + Z - 1, Z)
    mirror = Z - 1 - z
    mirror_e, mirror_w = lax.rem(mirror + 1, Z), lax.rem(mirror + Z - 1, Z)
    rows = nx + 2 * PAD
    width = ny + LANES
    last = ny - LANES
    own = slice(PAD, PAD + nx)
    lane = iota((nx, LANES), 1)

    moves = (
        (thick_any, thick),
        (faces_any, faces),
        (height_any, X.at[0, own, 0:ny]),
        (trans_u_any, X.at[1, own, 0:ny]),
        (trans_v_any, X.at[2, own, 0:ny]),
        (base_any, X.at[6:8, own, 0:ny]),
        (vel_u_any, vel_u),
        (vel_v_any, vel_v),
        (seeds_any, seeds),
        (scale_any, scale),
    )
    loads = [pltpu.make_async_copy(src, dst, load_sem.at[k]) for k, (src, dst) in enumerate(moves)]
    for load in loads:
        load.start()

    barrier = pltpu.get_barrier_semaphore()
    for zz, mm in ((left, m), (right, m), (left, other), (right, other), (z, other)):
        pl.semaphore_signal(barrier, inc=1, device_id={"zonal": zz, "merid": mm}, device_id_type=MESH)
    for zz in (mirror_w, mirror, mirror_e):

        @pl.when(jnp.logical_and(top, zz != z))
        def _():
            pl.semaphore_signal(barrier, inc=1, device_id={"zonal": zz}, device_id_type=MESH)

    loads[1].wait()
    X[3, own, 0:ny] = faces[0].astype(jnp.float32)
    X[4, own, 0:ny] = faces[1].astype(jnp.float32)
    loads[0].wait()
    total = thick[0]
    for l in range(1, layers):
        total = total + thick[l]
    X[5, own, 0:ny] = (WAVE_LIMIT / layers) * total

    def pack_tile(step, fields):
        at = 0
        for f in range(fields):
            west_send[step, at : at + WEST[f], :] = X[f, PAD + nx - WEST[f] : PAD + nx, 0:ny]
            at += WEST[f]
        at = 0
        for f in range(fields):
            east_send[step, at : at + EAST[f], :] = X[f, PAD : PAD + EAST[f], 0:ny]
            at += EAST[f]
        inner = jnp.zeros((nx, LANES), jnp.float32)
        crest = jnp.zeros((nx, LANES), jnp.float32)
        for f in range(fields):
            here = jnp.logical_and(lane >= f * SLOT, lane < (f + 1) * SLOT)
            high = roll(X[f, own, last:ny], SLOT * (f + 1), 1)
            low = roll(X[f, own, 0:LANES], SLOT * f, 1)
            crest = jnp.where(here, high, crest)
            inner = jnp.where(here, jnp.where(bottom, high, low), inner)
        pack_send[step, 0] = inner
        pack_send[step, 2] = crest
        for r in range(nx):
            pack_send[step, 1, r : r + 1, :] = pack_send[step, 2, nx - 1 - r : nx - r, :]

    def send_tile(step, fields):
        def send(src, dst, k, zz, mm):
            return pltpu.make_async_remote_copy(
                src_ref=src,
                dst_ref=dst,
                send_sem=send_sem.at[step, k],
                recv_sem=recv_sem.at[step, k],
                device_id={"zonal": zz, "merid": mm},
                device_id_type=MESH,
            )

        west, east = tile_up(sum(WEST[:fields])), tile_up(sum(EAST[:fields]))
        tail, whole, start = slice(nx - PAD, nx), slice(0, nx), slice(0, PAD)
        places = (slice(0, PAD), own, slice(PAD + nx, rows))
        inner = lambda s, part: (pack_send.at[step, 0, part], inner_recv.at[step, places[s]])
        copies = [
            send(*inner(2, start), 4, left, other),
            send(*inner(1, whole), 5, z, other),
            send(*inner(0, tail), 6, right, other),
            send(west_send.at[step, 0:west], west_recv.at[step, 0:west], 0, right, m),
            send(east_send.at[step, 0:east], east_recv.at[step, 0:east], 1, left, m),
        ]
        folds = []
        for s, part, zz in ((2, start, mirror_w), (1, whole, mirror), (0, tail, mirror_e)):
            src, dst = pack_send.at[step, 1, part], fold_recv.at[step, places[s]]
            near = pltpu.make_async_copy(src, dst, recv_sem.at[step, 7 + s])
            folds.append((send(src, dst, 7 + s, zz, m), near, zz))
        for far_copy, near_copy, zz in folds:

            @pl.when(jnp.logical_and(top, zz != z))
            def _():
                far_copy.start()

            @pl.when(jnp.logical_and(top, zz == z))
            def _():
                near_copy.start()

        for copy in copies:
            copy.start()
        return copies, folds

    def take_tile(step, fields, copies, folds):
        for copy in copies:
            copy.wait()
        for far_copy, near_copy, zz in folds:

            @pl.when(jnp.logical_and(top, zz != z))
            def _():
                far_copy.wait()

            @pl.when(jnp.logical_and(top, zz == z))
            def _():
                near_copy.wait()

        at = 0
        for f in range(fields):
            X[f, PAD - WEST[f] : PAD, 0:ny] = west_recv[step, at : at + WEST[f], :]
            at += WEST[f]
        at = 0
        for f in range(fields):
            X[f, PAD + nx : PAD + nx + EAST[f], 0:ny] = east_recv[step, at : at + EAST[f], :]
            at += EAST[f]
        for f in range(fields):
            got = inner_recv[step]
            X[f, :, ny:width] = jnp.where(
                top, roll(got, LANES - SLOT * (f + 1), 1), roll(got, LANES - SLOT * f, 1)
            )
            G[f] = roll(fold_recv[step], LANES - SLOT * (f + 1), 1)

    for load in loads[2:6]:
        load.wait()
    pack_tile(0, FIELDS)
    across = sum((zz != z).astype(jnp.int32) for zz in (mirror_w, mirror, mirror_e))
    pl.semaphore_wait(barrier, 5 + jnp.where(top, across, 0))
    tile = send_tile(0, FIELDS)

    def lay_copies(step):
        def one(src, dst, k, zz, mm):
            return pltpu.make_async_remote_copy(
                src_ref=src,
                dst_ref=dst,
                send_sem=lay_send_sem.at[step, k],
                recv_sem=lay_recv_sem.at[step, k],
                device_id={"zonal": zz, "merid": mm},
                device_id_type=MESH,
            )

        return [
            one(lay_send_r.at[step], lay_recv_w.at[step], 0, right, m),
            one(lay_send_l.at[step], lay_recv_e.at[step], 1, left, m),
            one(lay_pack_send.at[step, 0], lay_pack_recv.at[step, 0], 2, z, other),
            one(lay_pack_send.at[step, 1], lay_pack_recv.at[step, 1], 3, mirror, m),
        ]

    above = lay_send_r.shape[1] // 2

    def send_layers(step, h_ref, u_ref, v_ref):
        edge = jnp.zeros((nx, LANES), jnp.float32)
        brim = jnp.zeros((nx, LANES), jnp.float32)
        for l in range(layers):
            lay_send_r[step, l : l + 1, :] = h_ref[l, nx - 1 : nx, :]
            lay_send_r[step, above + l : above + l + 1, :] = u_ref[l, nx - 1 : nx, :]
            lay_send_l[step, l : l + 1, :] = h_ref[l, 0:1, :]
            high = roll(h_ref[l, :, last:ny], l + 1, 1)
            low = roll(h_ref[l, :, 0:LANES], l, 1)
            high_v = roll(v_ref[l, :, last:ny], layers + l + 1, 1)
            edge = jnp.where(lane == l, jnp.where(bottom, high, low), edge)
            edge = jnp.where(lane == layers + l, high_v, edge)
            brim = jnp.where(lane == l, high, brim)
        lay_pack_send[step, 0] = edge
        lay_pack_send[step, 2] = brim
        for r in range(nx):
            lay_pack_send[step, 1, r : r + 1, :] = lay_pack_send[step, 2, nx - 1 - r : nx - r, :]
        out = lay_copies(step)
        for copy in out[:3]:
            copy.start()

        @pl.when(top)
        def _():
            out[3].start()

        return out

    def wait_layers(out):
        for copy in out[:3]:
            copy.wait()

        @pl.when(top)
        def _():
            out[3].wait()

    for load in loads[6:]:
        load.wait()
    out = send_layers(0, thick, vel_u, vel_v)

    first = (z * nx - PAD).astype(jnp.float32)
    col = first + iota((rows, 1), 0).astype(jnp.float32) + float(total_x)
    far_col = float(2 * total_x - 1) - (first + iota((rows, 1), 0).astype(jnp.float32))
    spot = iota((1, width), 1)
    row = spot + m * ny
    row = jnp.where(jnp.logical_and(top, spot >= ny), row - width, row).astype(jnp.float32)
    far_row = (iota((1, LANES), 1) + (total_y - LANES)).astype(jnp.float32)
    px = jnp.zeros((rows, width), jnp.float32)
    py = jnp.zeros((rows, width), jnp.float32)
    fx = jnp.zeros((rows, LANES), jnp.float32)
    fy = jnp.zeros((rows, LANES), jnp.float32)
    for k in range(seeds.shape[1]):
        seed_x = seeds[0, k].astype(jnp.float32)
        seed_y = seeds[1, k].astype(jnp.float32)
        ca, sa = turns(seed_x, col, total_x)
        cf, sf = turns(seed_x, far_col, total_x)
        cb, sb = turns(seed_y, row, total_y)
        cg, sg = turns(seed_y, far_row, total_y)
        amp = scale[k]
        ca, sa, cf, sf = amp * ca, amp * sa, amp * cf, amp * sf
        px = px + (ca * cb - sa * sb)
        py = py + (sa * cb + ca * sb)
        fx = fx + (cf * cg - sf * sg)
        fy = fy + (sf * cg + cf * sg)
    wind_own[0] = px
    wind_own[1] = py
    wind_far[0] = fx
    wind_far[1] = fy

    take_tile(0, FIELDS, *tile)
    for k in range(2):
        X[6 + k] = STRESS_SCALE * (X[6 + k] + wind_own[k])
        G[6 + k] = STRESS_SCALE * (G[6 + k] + wind_far[k])

    lanes = iota((rows, width), 1)
    wall = jnp.logical_and(bottom, lanes == 0)
    crown = jnp.logical_and(top, lanes == ny - 1)
    far_top = iota((rows, LANES), 1) == LANES - 1

    def substep(_, carry):
        eta, bu, bv = X[0], X[1], X[2]
        g_eta, g_bu, g_bv = G[0], G[1], G[2]
        eta = eta - (bu - roll(bu, 1, 0) + bv - jnp.where(wall, 0.0, roll(bv, 1, 1)))
        g_eta = g_eta - (g_bu - roll(g_bu, -1, 0) + g_bv - roll(g_bv, 1, 1))
        north = jnp.where(crown, g_eta[:, LANES - 1 :], roll(eta, -1, 1))
        g_north = jnp.where(far_top, eta[:, ny - 1 : ny], roll(g_eta, -1, 1))
        bu = X[3] * (bu - X[5] * (roll(eta, -1, 0) - eta) + X[6])
        bv = X[4] * (bv - X[5] * (north - eta) + X[7])
        g_bu = G[3] * (g_bu - G[5] * (roll(g_eta, 1, 0) - g_eta) + G[6])
        g_bv = G[4] * (g_bv - G[5] * (g_north - g_eta) + G[7])
        X[0], X[1], X[2] = eta, bu, bv
        G[0], G[1], G[2] = g_eta, g_bu, g_bv
        aux[3] = aux[3] + bu[own, 0:ny]
        aux[4] = aux[4] + bv[own, 0:ny]
        return carry

    def substeps():
        aux[3:5] = jnp.zeros((2, nx, ny), jnp.float32)
        lax.fori_loop(0, NSUB, substep, 0)

    aux[7] = X[3, own, 0:ny]
    aux[8] = X[4, own, 0:ny]
    h_ref, u_ref, v_ref = thick, vel_u, vel_v
    for step in range(STEPS - 1):
        substeps()
        pack_tile(step + 1, 3)
        tile = send_tile(step + 1, 3)
        wait_layers(out)
        layer_step(
            h_ref, u_ref, v_ref, lay_recv_w.at[step], lay_recv_e.at[step], lay_pack_recv.at[step],
            aux.at[3:5], aux[7], aux[8], aux.at[5:7], o_h, o_u, o_v, top, step == 0, lambda k: None,
        )
        h_ref, u_ref, v_ref = o_h, o_u, o_v
        out = send_layers(step + 1, o_h, o_u, o_v)
        take_tile(step + 1, 3, *tile)
    substeps()
    for f in range(3):
        aux[f] = X[f, own, 0:ny]
    wait_layers(out)
    o_recv_w[...] = lay_recv_w[STEPS - 1]
    o_recv_e[...] = lay_recv_e[STEPS - 1]
    o_packs[...] = lay_pack_recv[STEPS - 1]


def body(zonal_devices, merid_devices, *args):
    thickness = args[3]
    layers, nx, ny = thickness.shape
    up = tile_up(layers)
    f32 = jnp.float32
    vmem = pl.BlockSpec(memory_space=pltpu.VMEM)
    far = pl.BlockSpec(memory_space=pltpu.HBM)
    hbm = pl.BlockSpec(memory_space=pl.ANY)
    rows = nx + 2 * PAD
    west, east = tile_up(sum(WEST)), tile_up(sum(EAST))
    plane = jax.ShapeDtypeStruct((nx, ny), f32)
    solid = jax.ShapeDtypeStruct((layers, nx, ny), f32)
    kept = [
        (9, nx, ny), (layers, nx, ny), (layers, nx, ny), (layers, nx, ny), (2 * up, ny), (up, ny), (2, nx, LANES),
    ]
    room = sum(math.prod(shape) for shape in kept)
    args = list(args)
    args[7] = args[7].T
    between = pl.pallas_call(
        functools.partial(kernel, zonal_devices, merid_devices),
        out_shape=[pltpu.VMEM(shape, f32) for shape in kept],
        in_specs=[far] * 10,
        out_specs=[vmem] * len(kept),
        scratch_shapes=[
            pltpu.VMEM((layers, nx, ny), f32),
            pltpu.VMEM((layers, nx, ny), f32),
            pltpu.VMEM((layers, nx, ny), f32),
            pltpu.VMEM((2, nx, ny), jnp.int32),
            pltpu.SMEM(args[7].shape, jnp.int32),
            pltpu.SMEM(args[8].shape, f32),
            pltpu.VMEM((FIELDS, rows, ny + LANES), f32),
            pltpu.VMEM((FIELDS, rows, LANES), f32),
            pltpu.VMEM((2, rows, ny + LANES), f32),
            pltpu.VMEM((2, rows, LANES), f32),
            pltpu.VMEM((STEPS, west, ny), f32),
            pltpu.VMEM((STEPS, west, ny), f32),
            pltpu.VMEM((STEPS, east, ny), f32),
            pltpu.VMEM((STEPS, east, ny), f32),
            pltpu.VMEM((STEPS, 3, nx, LANES), f32),
            pltpu.VMEM((STEPS, rows, LANES), f32),
            pltpu.VMEM((STEPS, rows, LANES), f32),
            pltpu.VMEM((STEPS, 2 * up, ny), f32),
            pltpu.VMEM((STEPS, up, ny), f32),
            pltpu.VMEM((STEPS, 2 * up, ny), f32),
            pltpu.VMEM((STEPS, up, ny), f32),
            pltpu.VMEM((STEPS, 3, nx, LANES), f32),
            pltpu.VMEM((STEPS, 2, nx, LANES), f32),
            pltpu.SemaphoreType.DMA((10,)),
            pltpu.SemaphoreType.DMA((STEPS, 10)),
            pltpu.SemaphoreType.DMA((STEPS, 10)),
            pltpu.SemaphoreType.DMA((STEPS, 4)),
            pltpu.SemaphoreType.DMA((STEPS, 4)),
        ],
        compiler_params=pltpu.CompilerParams(
            collective_id=0, has_side_effects=True, vmem_limit_bytes=VMEM_BYTES - 4 * room - SPARE
        ),
        name="ocean",
    )(*args)
    return pl.pallas_call(
        last_kernel,
        out_shape=(plane, plane, plane, solid, solid, solid),
        in_specs=[vmem] * len(kept),
        out_specs=[hbm] * 6,
        scratch_shapes=[
            pltpu.VMEM((layers, nx, ny), f32),
            pltpu.VMEM((layers, nx, ny), f32),
            pltpu.VMEM((layers, nx, ny), f32),
            pltpu.SemaphoreType.DMA((6,)),
        ],
        compiler_params=pltpu.CompilerParams(vmem_limit_bytes=24 * 1024 * 1024),
        name="last",
    )(*between)


def solution(mesh):
    field = P(("members", "zonal"), "merid")
    solid = P(None, ("members", "zonal"), "merid")
    fixed = P(None, "zonal", "merid")
    return jax.shard_map(
        functools.partial(body, mesh.shape["zonal"], mesh.shape["merid"]),
        mesh=mesh,
        in_specs=(
            field, field, field, solid, solid, solid, fixed, P("members", None), P("members"), fixed,
        ),
        out_specs=(field, field, field, solid, solid, solid),
        check_vma=False,
    )
```

```python
import functools
import math

import jax
import jax.numpy as jnp
from jax import lax
from jax.experimental import pallas as pl
from jax.experimental.pallas import tpu as pltpu
from jax.sharding import PartitionSpec as P

NSUB = 6
STEPS = 2
MARGIN = NSUB
PAD = 8

WAVE_LIMIT = 0.225
STRESS_SCALE = 0.1
FLUX_STEP = 0.05
PRESS_COEF = 0.05
LANES = 128
VMEM_BYTES = 67043328
SPARE = 1 << 15
FIELDS = 8
SLOT = LANES // FIELDS
WEST = (NSUB - 1, NSUB, NSUB - 1, NSUB - 1, NSUB - 2, NSUB - 1, NSUB - 1, NSUB - 2)
EAST = (NSUB, NSUB, NSUB) + (NSUB - 1,) * 5
ORDER = (0, 1, 2, 3, 4, 6, 7, 5)
CUT = 32
MESH = pl.DeviceIdType.MESH


def roll(value, shift, axis):
    return pltpu.roll(value, shift % value.shape[axis], axis)


def iota(shape, axis):
    return lax.broadcasted_iota(jnp.int32, shape, axis)


def turns(seed, index, total):
    part = seed * index * (1.0 / total)
    angle = (2.0 * math.pi) * (part - jnp.floor(part))
    return jnp.cos(angle), jnp.sin(angle)


def tile_up(count):
    return -(-count // 8) * 8


def layer_step(h_ref, u_ref, v_ref, recv_w, recv_e, packs, mean, mask_u, mask_v, depth, o_h, o_u, o_v, top, deep, sent):
    layers, nx, ny = h_ref.shape
    above = recv_w.shape[0] // 2
    row_id = iota((nx, ny), 0)
    lane_id = iota((nx, ny), 1)
    at_west = row_id == 0
    at_east = row_id == nx - 1
    at_south = lane_id == 0
    at_north = lane_id == ny - 1
    zero = jnp.zeros((nx, ny), jnp.float32)
    press_u, press_v, sum_u, sum_v = zero, zero, zero, zero
    deep_u, deep_v = zero, zero
    for l in range(layers):
        h, u, v = h_ref[l], u_ref[l], v_ref[l]
        side = packs[0, :, l : l + 1]
        cap = jnp.where(top, packs[1, :, l : l + 1], side)
        south_v = packs[0, :, layers + l : layers + l + 1]
        h_east = jnp.where(at_east, recv_e[l : l + 1, :], roll(h, -1, 0))
        h_north = jnp.where(at_north, cap, roll(h, -1, 1))
        hu = (h + h_east) * 0.5
        hv = (h + h_north) * 0.5
        if deep:
            deep_u = deep_u + hu
            deep_v = deep_v + hv
        flux_u = u * hu
        flux_v = v * hv
        west_row = recv_w[above + l : above + l + 1, :] * ((recv_w[l : l + 1, :] + h[0:1, :]) * 0.5)
        south_col = jnp.where(top, south_v * ((side + h[:, 0:1]) * 0.5), 0.0)
        flux_w = jnp.where(at_west, west_row, roll(flux_u, 1, 0))
        flux_s = jnp.where(at_south, south_col, roll(flux_v, 1, 1))
        press_u = press_u + (h_east - h)
        press_v = press_v + (h_north - h)
        trial_u = u - PRESS_COEF * press_u
        trial_v = v - PRESS_COEF * press_v
        sum_u = sum_u + hu * trial_u
        sum_v = sum_v + hv * trial_v
        o_u[l] = trial_u
        o_v[l] = trial_v
        o_h[l] = h - FLUX_STEP * (flux_u - flux_w + flux_v - flux_s)
    sent(0)
    if deep:
        depth[0] = 1.0 / deep_u
        depth[1] = 1.0 / deep_v
    fix_u = (mean[0] * (1.0 / NSUB) - sum_u) * depth[0]
    fix_v = (mean[1] * (1.0 / NSUB) - sum_v) * depth[1]
    for l in range(layers):
        o_u[l] = mask_u * (o_u[l] + fix_u)
    sent(1)
    for l in range(layers):
        o_v[l] = mask_v * (o_v[l] + fix_v)
    sent(2)


def last_kernel(
    aux, h_ref, u_ref, v_ref, recv_w, recv_e, packs, o_eta, o_bu, o_bv, o_h, o_u, o_v, n_h, n_u, n_v, sems
):
    top = lax.axis_index("merid") == lax.axis_size("merid") - 1
    flat = [pltpu.make_async_copy(aux.at[k], o, sems.at[3 + k]) for k, o in enumerate((o_eta, o_bu, o_bv))]
    for copy in flat:
        copy.start()
    out = [pltpu.make_async_copy(n, o, sems.at[k]) for k, (n, o) in enumerate(((n_h, o_h), (n_u, o_u), (n_v, o_v)))]
    layer_step(
        h_ref, u_ref, v_ref, recv_w, recv_e, packs, aux.at[3:5], aux[7], aux[8], aux.at[5:7],
        n_h, n_u, n_v, top, False, lambda k: out[k].start(),
    )
    for copy in flat + out:
        copy.wait()


def kernel(
    zonal_devices,
    merid_devices,
    height_any,
    trans_u_any,
    trans_v_any,
    thick_any,
    vel_u_any,
    vel_v_any,
    faces_any,
    seeds_any,
    scale_any,
    base_any,
    aux,
    o_h,
    o_u,
    o_v,
    o_recv_w,
    o_recv_e,
    o_packs,
    thick,
    vel_u,
    vel_v,
    faces,
    seeds,
    scale,
    X,
    G,
    wind_own,
    wind_far,
    west_send,
    west_recv,
    east_send,
    east_recv,
    pack_send,
    inner_recv,
    fold_recv,
    lay_send_r,
    lay_send_l,
    lay_recv_w,
    lay_recv_e,
    lay_pack_send,
    lay_pack_recv,
    load_sem,
    send_sem,
    recv_sem,
    lay_send_sem,
    lay_recv_sem,
):
    layers, nx, ny = thick.shape
    Z = zonal_devices
    total_x, total_y = nx * Z, ny * merid_devices
    z = lax.axis_index("zonal")
    m = lax.axis_index("merid")
    other = 1 - m
    bottom = m == 0
    top = m == merid_devices - 1
    right, left = lax.rem(z + 1, Z), lax.rem(z + Z - 1, Z)
    mirror = Z - 1 - z
    mirror_e, mirror_w = lax.rem(mirror + 1, Z), lax.rem(mirror + Z - 1, Z)
    rows = nx + 2 * PAD
    width = ny + LANES
    last = ny - LANES
    own = slice(PAD, PAD + nx)
    lane = iota((nx, LANES), 1)

    barrier = pltpu.get_barrier_semaphore()
    for zz, mm in ((left, m), (right, m), (left, other), (right, other), (z, other)):
        pl.semaphore_signal(barrier, inc=1, device_id={"zonal": zz, "merid": mm}, device_id_type=MESH)
    for zz in (mirror_w, mirror, mirror_e):

        @pl.when(jnp.logical_and(top, zz != z))
        def _():
            pl.semaphore_signal(barrier, inc=1, device_id={"zonal": zz}, device_id_type=MESH)

    moves = (
        (faces_any, faces),
        (height_any, X.at[0, own, 0:ny]),
        (trans_u_any, X.at[1, own, 0:ny]),
        (trans_v_any, X.at[2, own, 0:ny]),
        (base_any, X.at[6:8, own, 0:ny]),
        (thick_any, thick),
        (vel_u_any, vel_u),
        (vel_v_any, vel_v),
        (seeds_any, seeds),
        (scale_any, scale),
    )
    loads = [pltpu.make_async_copy(src, dst, load_sem.at[k]) for k, (src, dst) in enumerate(moves)]
    for load in loads:
        load.start()

    loads[0].wait()
    X[3, own, 0:ny] = faces[0].astype(jnp.float32)
    X[4, own, 0:ny] = faces[1].astype(jnp.float32)
    for load in loads[1:5]:
        load.wait()

    def pack_rows(step, start, stop):
        west = sum(WEST[f] for f in ORDER[:start])
        east = sum(EAST[f] for f in ORDER[:start])
        for f in ORDER[start:stop]:
            west_send[step, west : west + WEST[f], :] = X[f, PAD + nx - WEST[f] : PAD + nx, 0:ny]
            east_send[step, east : east + EAST[f], :] = X[f, PAD : PAD + EAST[f], 0:ny]
            west += WEST[f]
            east += EAST[f]

    def pack_edges(step, fields):
        inner = jnp.zeros((nx, LANES), jnp.float32)
        crest = jnp.zeros((nx, LANES), jnp.float32)
        for f in range(fields):
            here = jnp.logical_and(lane >= f * SLOT, lane < (f + 1) * SLOT)
            high = roll(X[f, own, last:ny], SLOT * (f + 1), 1)
            low = roll(X[f, own, 0:LANES], SLOT * f, 1)
            crest = jnp.where(here, high, crest)
            inner = jnp.where(here, jnp.where(bottom, high, low), inner)
        pack_send[step, 0] = inner
        pack_send[step, 2] = crest
        for r in range(nx):
            pack_send[step, 1, r : r + 1, :] = pack_send[step, 2, nx - 1 - r : nx - r, :]

    def send_tile(step, fields):
        def send(src, dst, k, zz, mm):
            return pltpu.make_async_remote_copy(
                src_ref=src,
                dst_ref=dst,
                send_sem=send_sem.at[step, k],
                recv_sem=recv_sem.at[step, k],
                device_id={"zonal": zz, "merid": mm},
                device_id_type=MESH,
            )

        bulk = []
        for src, dst, k, zz, count in (
            (west_send, west_recv, 0, right, tile_up(sum(WEST[:fields]))),
            (east_send, east_recv, 1, left, tile_up(sum(EAST[:fields]))),
        ):
            cuts = [0, CUT, count] if count > CUT else [0, count]
            for n, (low, high) in enumerate(zip(cuts[:-1], cuts[1:])):
                part = slice(low, high)
                bulk.append((n, send(src.at[step, part], dst.at[step, part], k + 2 * n, zz, m)))
        tail, whole, start = slice(nx - PAD, nx), slice(0, nx), slice(0, PAD)
        places = (slice(0, PAD), own, slice(PAD + nx, rows))
        inner = lambda s, part: (pack_send.at[step, 0, part], inner_recv.at[step, places[s]])
        copies = [
            send(*inner(2, start), 4, left, other),
            send(*inner(1, whole), 5, z, other),
            send(*inner(0, tail), 6, right, other),
        ]
        folds = []
        for s, part, zz in ((2, start, mirror_w), (1, whole, mirror), (0, tail, mirror_e)):
            src, dst = pack_send.at[step, 1, part], fold_recv.at[step, places[s]]
            near = pltpu.make_async_copy(src, dst, recv_sem.at[step, 7 + s])
            folds.append((send(src, dst, 7 + s, zz, m), near, zz))
        return [c for n, c in bulk if n == 0], [c for n, c in bulk if n > 0] + copies, folds

    def start_rest(copies, folds):
        for far_copy, near_copy, zz in folds:

            @pl.when(jnp.logical_and(top, zz != z))
            def _():
                far_copy.start()

            @pl.when(jnp.logical_and(top, zz == z))
            def _():
                near_copy.start()

        for copy in copies:
            copy.start()

    def take_tile(step, fields, bulk, copies, folds):
        for copy in bulk + copies:
            copy.wait()
        for far_copy, near_copy, zz in folds:

            @pl.when(jnp.logical_and(top, zz != z))
            def _():
                far_copy.wait()

            @pl.when(jnp.logical_and(top, zz == z))
            def _():
                near_copy.wait()

        west = east = 0
        for f in ORDER[:fields]:
            X[f, PAD - WEST[f] : PAD, 0:ny] = west_recv[step, west : west + WEST[f], :]
            X[f, PAD + nx : PAD + nx + EAST[f], 0:ny] = east_recv[step, east : east + EAST[f], :]
            west += WEST[f]
            east += EAST[f]
        for f in range(fields):
            got = inner_recv[step]
            X[f, :, ny:width] = jnp.where(
                top, roll(got, LANES - SLOT * (f + 1), 1), roll(got, LANES - SLOT * f, 1)
            )
            G[f] = roll(fold_recv[step], LANES - SLOT * (f + 1), 1)

    def post_bulk(tile):
        for copy in tile[0]:
            copy.start()

    pack_rows(0, 0, FIELDS - 1)
    across = sum((zz != z).astype(jnp.int32) for zz in (mirror_w, mirror, mirror_e))
    pl.semaphore_wait(barrier, 5 + jnp.where(top, across, 0))
    tile = send_tile(0, FIELDS)
    post_bulk(tile)
    loads[5].wait()
    total = thick[0]
    for l in range(1, layers):
        total = total + thick[l]
    X[5, own, 0:ny] = (WAVE_LIMIT / layers) * total
    pack_rows(0, FIELDS - 1, FIELDS)
    pack_edges(0, FIELDS)
    start_rest(*tile[1:])

    def lay_copies(step):
        def one(src, dst, k, zz, mm):
            return pltpu.make_async_remote_copy(
                src_ref=src,
                dst_ref=dst,
                send_sem=lay_send_sem.at[step, k],
                recv_sem=lay_recv_sem.at[step, k],
                device_id={"zonal": zz, "merid": mm},
                device_id_type=MESH,
            )

        return [
            one(lay_send_r.at[step], lay_recv_w.at[step], 0, right, m),
            one(lay_send_l.at[step], lay_recv_e.at[step], 1, left, m),
            one(lay_pack_send.at[step, 0], lay_pack_recv.at[step, 0], 2, z, other),
            one(lay_pack_send.at[step, 1], lay_pack_recv.at[step, 1], 3, mirror, m),
        ]

    above = lay_send_r.shape[1] // 2

    def send_layers(step, h_ref, u_ref, v_ref):
        edge = jnp.zeros((nx, LANES), jnp.float32)
        brim = jnp.zeros((nx, LANES), jnp.float32)
        for l in range(layers):
            lay_send_r[step, l : l + 1, :] = h_ref[l, nx - 1 : nx, :]
            lay_send_r[step, above + l : above + l + 1, :] = u_ref[l, nx - 1 : nx, :]
            lay_send_l[step, l : l + 1, :] = h_ref[l, 0:1, :]
            high = roll(h_ref[l, :, last:ny], l + 1, 1)
            low = roll(h_ref[l, :, 0:LANES], l, 1)
            high_v = roll(v_ref[l, :, last:ny], layers + l + 1, 1)
            edge = jnp.where(lane == l, jnp.where(bottom, high, low), edge)
            edge = jnp.where(lane == layers + l, high_v, edge)
            brim = jnp.where(lane == l, high, brim)
        lay_pack_send[step, 0] = edge
        lay_pack_send[step, 2] = brim
        for r in range(nx):
            lay_pack_send[step, 1, r : r + 1, :] = lay_pack_send[step, 2, nx - 1 - r : nx - r, :]
        out = lay_copies(step)
        for copy in out[:3]:
            copy.start()

        @pl.when(top)
        def _():
            out[3].start()

        return out

    def wait_layers(out):
        for copy in out[:3]:
            copy.wait()

        @pl.when(top)
        def _():
            out[3].wait()

    for load in loads[6:]:
        load.wait()
    out = send_layers(0, thick, vel_u, vel_v)

    first = (z * nx - PAD).astype(jnp.float32)
    col = first + iota((rows, 1), 0).astype(jnp.float32) + float(total_x)
    far_col = float(2 * total_x - 1) - (first + iota((rows, 1), 0).astype(jnp.float32))
    spot = iota((1, width), 1)
    row = spot + m * ny
    row = jnp.where(jnp.logical_and(top, spot >= ny), row - width, row).astype(jnp.float32)
    far_row = (iota((1, LANES), 1) + (total_y - LANES)).astype(jnp.float32)
    px = jnp.zeros((rows, width), jnp.float32)
    py = jnp.zeros((rows, width), jnp.float32)
    fx = jnp.zeros((rows, LANES), jnp.float32)
    fy = jnp.zeros((rows, LANES), jnp.float32)
    for k in range(seeds.shape[1]):
        seed_x = seeds[0, k].astype(jnp.float32)
        seed_y = seeds[1, k].astype(jnp.float32)
        ca, sa = turns(seed_x, col, total_x)
        cf, sf = turns(seed_x, far_col, total_x)
        cb, sb = turns(seed_y, row, total_y)
        cg, sg = turns(seed_y, far_row, total_y)
        amp = scale[k]
        ca, sa, cf, sf = amp * ca, amp * sa, amp * cf, amp * sf
        px = px + (ca * cb - sa * sb)
        py = py + (sa * cb + ca * sb)
        fx = fx + (cf * cg - sf * sg)
        fy = fy + (sf * cg + cf * sg)
    wind_own[0] = px
    wind_own[1] = py
    wind_far[0] = fx
    wind_far[1] = fy

    take_tile(0, FIELDS, *tile)
    for k in range(2):
        X[6 + k] = STRESS_SCALE * (X[6 + k] + wind_own[k])
        G[6 + k] = STRESS_SCALE * (G[6 + k] + wind_far[k])

    lanes = iota((rows, width), 1)
    wall = jnp.logical_and(bottom, lanes == 0)
    crown = jnp.logical_and(top, lanes == ny - 1)
    far_top = iota((rows, LANES), 1) == LANES - 1

    def substep(_, carry):
        eta, bu, bv = X[0], X[1], X[2]
        g_eta, g_bu, g_bv = G[0], G[1], G[2]
        eta = eta - (bu - roll(bu, 1, 0) + bv - jnp.where(wall, 0.0, roll(bv, 1, 1)))
        g_eta = g_eta - (g_bu - roll(g_bu, -1, 0) + g_bv - roll(g_bv, 1, 1))
        north = jnp.where(crown, g_eta[:, LANES - 1 :], roll(eta, -1, 1))
        g_north = jnp.where(far_top, eta[:, ny - 1 : ny], roll(g_eta, -1, 1))
        bu = X[3] * (bu - X[5] * (roll(eta, -1, 0) - eta) + X[6])
        bv = X[4] * (bv - X[5] * (north - eta) + X[7])
        g_bu = G[3] * (g_bu - G[5] * (roll(g_eta, 1, 0) - g_eta) + G[6])
        g_bv = G[4] * (g_bv - G[5] * (g_north - g_eta) + G[7])
        X[0], X[1], X[2] = eta, bu, bv
        G[0], G[1], G[2] = g_eta, g_bu, g_bv
        aux[3] = aux[3] + bu[own, 0:ny]
        aux[4] = aux[4] + bv[own, 0:ny]
        return carry

    def substeps():
        aux[3:5] = jnp.zeros((2, nx, ny), jnp.float32)
        lax.fori_loop(0, NSUB, substep, 0, unroll=True)

    aux[7] = X[3, own, 0:ny]
    aux[8] = X[4, own, 0:ny]
    h_ref, u_ref, v_ref = thick, vel_u, vel_v
    for step in range(STEPS - 1):
        substeps()
        pack_rows(step + 1, 0, 3)
        tile = send_tile(step + 1, 3)
        post_bulk(tile)
        pack_edges(step + 1, 3)
        start_rest(*tile[1:])
        wait_layers(out)
        layer_step(
            h_ref, u_ref, v_ref, lay_recv_w.at[step], lay_recv_e.at[step], lay_pack_recv.at[step],
            aux.at[3:5], aux[7], aux[8], aux.at[5:7], o_h, o_u, o_v, top, step == 0, lambda k: None,
        )
        h_ref, u_ref, v_ref = o_h, o_u, o_v
        out = send_layers(step + 1, o_h, o_u, o_v)
        take_tile(step + 1, 3, *tile)
    substeps()
    for f in range(3):
        aux[f] = X[f, own, 0:ny]
    wait_layers(out)
    o_recv_w[...] = lay_recv_w[STEPS - 1]
    o_recv_e[...] = lay_recv_e[STEPS - 1]
    o_packs[...] = lay_pack_recv[STEPS - 1]


def body(zonal_devices, merid_devices, *args):
    thickness = args[3]
    layers, nx, ny = thickness.shape
    up = tile_up(layers)
    f32 = jnp.float32
    vmem = pl.BlockSpec(memory_space=pltpu.VMEM)
    far = pl.BlockSpec(memory_space=pltpu.HBM)
    hbm = pl.BlockSpec(memory_space=pl.ANY)
    rows = nx + 2 * PAD
    west, east = tile_up(sum(WEST)), tile_up(sum(EAST))
    plane = jax.ShapeDtypeStruct((nx, ny), f32)
    solid = jax.ShapeDtypeStruct((layers, nx, ny), f32)
    kept = [
        (9, nx, ny), (layers, nx, ny), (layers, nx, ny), (layers, nx, ny), (2 * up, ny), (up, ny), (2, nx, LANES),
    ]
    room = sum(math.prod(shape) for shape in kept)
    args = list(args)
    args[7] = args[7].T
    between = pl.pallas_call(
        functools.partial(kernel, zonal_devices, merid_devices),
        out_shape=[pltpu.VMEM(shape, f32) for shape in kept],
        in_specs=[far] * 10,
        out_specs=[vmem] * len(kept),
        scratch_shapes=[
            pltpu.VMEM((layers, nx, ny), f32),
            pltpu.VMEM((layers, nx, ny), f32),
            pltpu.VMEM((layers, nx, ny), f32),
            pltpu.VMEM((2, nx, ny), jnp.int32),
            pltpu.SMEM(args[7].shape, jnp.int32),
            pltpu.SMEM(args[8].shape, f32),
            pltpu.VMEM((FIELDS, rows, ny + LANES), f32),
            pltpu.VMEM((FIELDS, rows, LANES), f32),
            pltpu.VMEM((2, rows, ny + LANES), f32),
            pltpu.VMEM((2, rows, LANES), f32),
            pltpu.VMEM((STEPS, west, ny), f32),
            pltpu.VMEM((STEPS, west, ny), f32),
            pltpu.VMEM((STEPS, east, ny), f32),
            pltpu.VMEM((STEPS, east, ny), f32),
            pltpu.VMEM((STEPS, 3, nx, LANES), f32),
            pltpu.VMEM((STEPS, rows, LANES), f32),
            pltpu.VMEM((STEPS, rows, LANES), f32),
            pltpu.VMEM((STEPS, 2 * up, ny), f32),
            pltpu.VMEM((STEPS, up, ny), f32),
            pltpu.VMEM((STEPS, 2 * up, ny), f32),
            pltpu.VMEM((STEPS, up, ny), f32),
            pltpu.VMEM((STEPS, 3, nx, LANES), f32),
            pltpu.VMEM((STEPS, 2, nx, LANES), f32),
            pltpu.SemaphoreType.DMA((10,)),
            pltpu.SemaphoreType.DMA((STEPS, 10)),
            pltpu.SemaphoreType.DMA((STEPS, 10)),
            pltpu.SemaphoreType.DMA((STEPS, 4)),
            pltpu.SemaphoreType.DMA((STEPS, 4)),
        ],
        compiler_params=pltpu.CompilerParams(
            collective_id=0, has_side_effects=True, vmem_limit_bytes=VMEM_BYTES - 4 * room - SPARE
        ),
        name="ocean",
    )(*args)
    return pl.pallas_call(
        last_kernel,
        out_shape=(plane, plane, plane, solid, solid, solid),
        in_specs=[vmem] * len(kept),
        out_specs=[hbm] * 6,
        scratch_shapes=[
            pltpu.VMEM((layers, nx, ny), f32),
            pltpu.VMEM((layers, nx, ny), f32),
            pltpu.VMEM((layers, nx, ny), f32),
            pltpu.SemaphoreType.DMA((6,)),
        ],
        compiler_params=pltpu.CompilerParams(vmem_limit_bytes=24 * 1024 * 1024),
        name="last",
    )(*between)


def solution(mesh):
    field = P(("members", "zonal"), "merid")
    solid = P(None, ("members", "zonal"), "merid")
    fixed = P(None, "zonal", "merid")
    return jax.shard_map(
        functools.partial(body, mesh.shape["zonal"], mesh.shape["merid"]),
        mesh=mesh,
        in_specs=(
            field, field, field, solid, solid, solid, fixed, P("members", None), P("members"), fixed,
        ),
        out_specs=(field, field, field, solid, solid, solid),
        check_vma=False,
    )
```
